32 devices in a mesh: grp: 8 (over z, x), row: 4 (over y, core).
Axes of the slice: x: 2, y: 2, z: 4, core: 2. Of those that a mesh axis runs over, the one named last changes fastest.
Arguments:
- gll_state: float32 [8, 32, 16, 4096], P(None, None, None, ('grp', 'row')), may hold values from -6 to 6
- metric: float32 [16, 4096], P(None, ('grp', 'row')), may hold values from 0.7 to 1.4
- phys_owner: int32 [4096, 4, 1], P(('grp', 'row')), may hold values from 0 to 7; in each aligned block of 512 rows (0 to 511, 512 to 1023, ..., all dimensions but the last counted through in order) at most 128 rows name the same one
- neighbours: int32 [4, 4096], P(None, ('grp', 'row')), may hold values from 0 to 4095, as said below
- phys_rate: float32 [32, 32768], P(None, ('grp', 'row')), may hold values from 0.2 to 2
- phys_forcing: float32 [32, 32768], P(None, ('grp', 'row')), may hold values from -6 to 6
- field_mix: float32 [8, 8], replicated, may hold values from -2 to 2
Outputs:
- gll_tend: float32 [8, 32, 16, 4096], P(None, None, None, ('grp', 'row'))
The draws below stay inside these ranges and needn't reach their ends.
Inputs may be any that keep to these rules, and one draw needn't show every extreme that they name: `phys_owner`: in the 512 rows of one device, no owner is named more than 128 times, and some owner reaches 128. `neighbours`: rows 0 and 1 of element e are e - 1 and e + 1, cyclically over 4096 elements; rows 2 and 3 lie 2 to 32 positions before and after e, cyclically, and some element has a neighbour exactly 32 positions away.
All inputs are finite; a program needn't handle non-finite values.
Results may differ from the reference program's by a relative error of at most 0.000094.
Values sent between devices are 32-bit elements; how exact they have to be, the bound alone decides.
No kernel may reach another device: no remote copies, remote signals or barrier semaphores. Data moves between devices by JAX's collectives and lax.ppermute only.
A program may use at most 64 MiB of HBM per device.

```python
import math
import jax
import jax.numpy as jnp
import numpy as np
from jax import lax

NF = 8
NLEV = 32
NODES = 16
E_DEV = 128
HALO = 32
CAP = 128
ELEMS = 4096
SLOTS = 32768
N_GRP = 8
N_ROW = 4


def draw_neighbours(key, part):
    first_key = jax.random.fold_in(key, 11)
    second_key = jax.random.fold_in(key, 23)
    elem_ids = jnp.arange(ELEMS, dtype=jnp.int32)
    south_step = jax.random.randint(first_key, (ELEMS,), 2, HALO + 1, dtype=jnp.int32)
    north_step = jax.random.randint(second_key, (ELEMS,), 2, HALO + 1, dtype=jnp.int32)
    north_step = jnp.where(elem_ids == 0, HALO, north_step)
    return jnp.stack([(elem_ids - 1) % ELEMS, (elem_ids + 1) % ELEMS, (elem_ids - south_step) % ELEMS, (elem_ids + north_step) % ELEMS]).astype(jnp.int32)


def shard_levels(own_key, dims, shards, smallest, top_value):
    def one(dim, blocks):
        heights = jax.random.uniform(jax.random.fold_in(jax.random.fold_in(own_key, 6), dim), (blocks,), jnp.float32, smallest / len(shards), top_value / len(shards))
        return jnp.repeat(jnp.exp(heights), dims[dim] // blocks).reshape((-1,) + (1,) * (len(dims) - dim - 1))

    gain = one(*shards[0])
    for cut in shards[1:]:
        gain = gain * one(*cut)
    return gain


def routed_block(stream_key, own, number, rows, number_of, top, most, lean):
    sequence = jax.random.permutation(stream_key, number_of)
    crowded, usual = portions_of(number_of, rows * top, most, lean, True), portions_of(number_of, rows * top, most, lean, False)
    places = jnp.arange(number_of)

    def named(tallies, turn):
        used = int((tallies > 0).sum())
        fixed = max(1, used // 4)
        moved = fixed + (places - fixed + turn * (used - fixed)) % max(1, number_of - fixed)
        return jnp.zeros((number_of,), jnp.int32).at[sequence[jnp.where(places < fixed, places, moved)]].set(jnp.asarray(tallies, jnp.int32))

    tallies = jnp.where(number % 4 == 0, named(crowded, number // 4), named(usual, number - number // 4 - 1))
    mixed = jax.random.permutation(jax.random.fold_in(own, 3), number_of)
    donor, sink = mixed[0:number_of // 2 * 2:2], mixed[1:number_of // 2 * 2:2]
    margin = jnp.minimum(tallies[donor] - 1, most - tallies[sink]) // 2
    margin = jnp.where((donor == sequence[0]) | (sink == sequence[0]) | (tallies[sink] == 0), 0, jnp.maximum(margin, 0))
    moved = jax.random.randint(jax.random.fold_in(own, 4), (number_of // 2,), 0, 1 << 20) % (margin + 1)
    tallies = tallies.at[donor].add(-moved).at[sink].add(moved)
    labels = jnp.searchsorted(jnp.cumsum(tallies), jnp.arange(rows * top), side="right").astype(jnp.int32)
    table = labels.reshape(top, rows).T
    table = table[jax.random.permutation(jax.random.fold_in(own, 1), rows)]
    turn = jax.random.randint(jax.random.fold_in(own, 2), (rows, 1), 0, top)
    return jnp.take_along_axis(table, (jnp.arange(top)[None, :] + turn) % top, axis=1)


def portions_of(amount, total, bound, lean, full):
    portions = [(1 << 20) // math.isqrt(grade ** lean) + 1 for grade in range(1, amount + 1)]
    largest = bound if full else min(bound, max(-(-total // amount), total * portions[0] // sum(portions)))
    least = 1 if total - largest >= amount - 1 else 0
    counts, rest = [largest] + [least] * (amount - 1), total - largest - least * (amount - 1)
    while rest > 0:
        free = [i for i in range(1, amount) if counts[i] < largest] or [i for i in range(1, amount) if counts[i] < bound]
        mass, left = sum([portions[i] for i in free]), rest
        for i in free:
            more = min(bound - counts[i], max(1, left * portions[i] // mass), rest)
            counts[i] = counts[i] + more
            rest = rest - more
    return np.array(counts)


def centred(stream_key, extent, width, limit, split=(), kind=jnp.bfloat16):
    loudness = shard_levels(stream_key, extent, split, -0.22, 0.18) if split else 1.0
    values = jax.random.normal(stream_key, extent, jnp.float32) * width * loudness
    return jnp.minimum(jnp.maximum(values, -limit), limit).astype(kind)


def setup_inputs(seed: int = 0) -> dict:
    streams_of = jax.random.split(jax.random.key(seed), 8)
    gll_state = centred(streams_of[0], (NF, NLEV, NODES, ELEMS), 1.0, 6.0, ((3, 32),), jnp.float32)
    metric = jnp.clip(jnp.exp(math.log(1.4) - 0.6931472 * jax.random.uniform(streams_of[1], (NODES, ELEMS), jnp.float32) ** shard_levels(streams_of[1], (NODES, ELEMS), ((1, 32),), -0.2, 0.2)), 0.7, 1.4)
    phys_owner_keys = jax.random.split(jax.random.fold_in(streams_of[2], 1), ELEMS * 4 // (4 * E_DEV))
    phys_owner_turns = jax.random.permutation(jax.random.fold_in(streams_of[2], 3), ELEMS * 4 // (4 * E_DEV))
    phys_owner = jax.vmap(lambda own, number: routed_block(jax.random.fold_in(streams_of[2], 2), own, number, 4 * E_DEV, N_GRP, 1, CAP, 2))(phys_owner_keys, phys_owner_turns).reshape((ELEMS, 4, 1))
    neighbours = draw_neighbours(jax.random.fold_in(streams_of[7], 71), 0)
    phys_rate = jnp.clip(jnp.exp(math.log(2.0) - 2.3025851 * jax.random.uniform(streams_of[4], (NLEV, SLOTS), jnp.float32) ** shard_levels(streams_of[4], (NLEV, SLOTS), ((1, 32),), -0.2, 0.2)), 0.2, 2.0)
    phys_forcing = centred(streams_of[5], (NLEV, SLOTS), 1.0, 6.0, ((1, 32),), jnp.float32)
    field_mix = centred(streams_of[6], (NF, NF), NF ** -0.5, 2.0, (), jnp.float32)
    return dict(gll_state=gll_state, metric=metric, phys_owner=phys_owner, neighbours=neighbours, phys_rate=phys_rate, phys_forcing=phys_forcing, field_mix=field_mix)


def lagrange_value(gll_nodes, node_index, point):
    value = 1.0
    for other_index in range(4):
        if other_index != node_index:
            value = value * (point - gll_nodes[other_index]) / (gll_nodes[node_index] - gll_nodes[other_index])
    return value

def remap_tables():
    gll_nodes = np.array([-1.0, -1.0 / np.sqrt(5.0), 1.0 / np.sqrt(5.0), 1.0])
    offset = 0.5 / np.sqrt(3.0)
    halves = np.zeros((2, 4))
    for node_index in range(4):
        left_sum = lagrange_value(gll_nodes, node_index, -0.5 - offset) + lagrange_value(gll_nodes, node_index, -0.5 + offset)
        right_sum = lagrange_value(gll_nodes, node_index, 0.5 - offset) + lagrange_value(gll_nodes, node_index, 0.5 + offset)
        halves[0, node_index] = 0.5 * left_sum
        halves[1, node_index] = 0.5 * right_sum
    cell_weights = (halves[None, :, None, :] * halves[:, None, :, None]).reshape(4, 16)
    interp_cols = np.stack([0.5 - gll_nodes, 0.5 + gll_nodes], axis=1)
    cell_to_node = (interp_cols[None, :, None, :] * interp_cols[:, None, :, None]).reshape(16, 4)
    node_x = np.tile(gll_nodes, 4)
    node_y = np.repeat(gll_nodes, 4)
    slope_weights = 0.5 * np.stack([np.maximum(0.0, -node_x), np.maximum(0.0, node_x), np.maximum(0.0, -node_y), np.maximum(0.0, node_y)], axis=1)
    return (jnp.asarray(cell_weights, jnp.float32), jnp.asarray(cell_to_node, jnp.float32), jnp.asarray(slope_weights, jnp.float32))

def to_cells(gll_state, metric):
    cell_weights, cell_to_node, slope_weights = remap_tables()
    weighted = cell_weights[:, :, None] * metric[None, :, :]
    cell_area = lax.optimization_barrier(jnp.sum(weighted, axis=1))
    cell_mass = jnp.einsum('cne,flne->flce', weighted, gll_state, precision=lax.Precision.HIGHEST)
    return cell_mass / cell_area[None, None]

def physics(cell_values, relax_rate, forcing, field_mix):
    mixed_fields = jnp.einsum('fg,g...->f...', field_mix, cell_values, precision=lax.Precision.HIGHEST)
    return relax_rate[None] * jnp.tanh(mixed_fields + forcing[None])

def to_nodes(tendency, neighbour_means):
    cell_weights, cell_to_node, slope_weights = remap_tables()
    own_mean = lax.optimization_barrier(jnp.mean(tendency, axis=2))
    reconstructed = jnp.einsum('nc,flce->flne', cell_to_node, tendency, precision=lax.Precision.HIGHEST)
    reconstructed = reconstructed + jnp.einsum('nk,flke->flne', slope_weights, neighbour_means - own_mean[:, :, None], precision=lax.Precision.HIGHEST)
    lower_bound = jnp.minimum(lax.optimization_barrier(jnp.min(tendency, axis=2)), lax.optimization_barrier(jnp.min(neighbour_means, axis=2)))
    upper_bound = jnp.maximum(lax.optimization_barrier(jnp.max(tendency, axis=2)), lax.optimization_barrier(jnp.max(neighbour_means, axis=2)))
    return jnp.clip(reconstructed, lower_bound[:, :, None], upper_bound[:, :, None])

def reference(gll_state, metric, phys_owner, neighbours, phys_rate, phys_forcing, field_mix):
    device_total = N_GRP * N_ROW
    cell_values = to_cells(gll_state, metric)
    owner_grp = phys_owner[:, :, 0].reshape(device_total, 4 * E_DEV)
    onehot = (owner_grp[:, :, None] == jnp.arange(N_GRP, dtype=jnp.int32)[None, None, :]).astype(jnp.int32)
    slot_rank = lax.optimization_barrier(jnp.sum((jnp.cumsum(onehot, axis=1) - onehot) * onehot, axis=2))
    device_index = jnp.arange(device_total, dtype=jnp.int32)[:, None]
    target = ((owner_grp * N_ROW + device_index % N_ROW) * (N_GRP * CAP) + device_index // N_ROW * CAP + slot_rank).astype(jnp.int32)
    target = target.reshape(device_total * E_DEV, 4).T
    relax_rate = phys_rate[:, target]
    forcing = phys_forcing[:, target]
    tendency = physics(cell_values, relax_rate, forcing, field_mix)
    own_mean = lax.optimization_barrier(jnp.mean(tendency, axis=2))
    neighbour_means = own_mean[:, :, neighbours]
    return to_nodes(tendency, neighbour_means)
```

```python
import jax
import jax.numpy as jnp
import ml_dtypes
import numpy as np
from jax import lax
from jax.experimental import pallas as pl
from jax.experimental.pallas import tpu as pltpu
from jax.sharding import PartitionSpec as P

HALO = 32
BF16 = jnp.bfloat16
F32 = jnp.float32


def lagrange_value(gll_nodes, node_index, point):
    value = 1.0
    for other_index in range(4):
        if other_index != node_index:
            value = (
                value
                * (point - gll_nodes[other_index])
                / (gll_nodes[node_index] - gll_nodes[other_index])
            )
    return value


def remap_tables():
    gll_nodes = np.array([-1.0, -1.0 / np.sqrt(5.0), 1.0 / np.sqrt(5.0), 1.0])
    offset = 0.5 / np.sqrt(3.0)
    halves = np.zeros((2, 4))
    for node_index in range(4):
        left_sum = lagrange_value(gll_nodes, node_index, -0.5 - offset) + lagrange_value(
            gll_nodes, node_index, -0.5 + offset
        )
        right_sum = lagrange_value(gll_nodes, node_index, 0.5 - offset) + lagrange_value(
            gll_nodes, node_index, 0.5 + offset
        )
        halves[0, node_index] = 0.5 * left_sum
        halves[1, node_index] = 0.5 * right_sum
    cell_weights = (halves[None, :, None, :] * halves[:, None, :, None]).reshape(4, 16)
    interp_cols = np.stack([0.5 - gll_nodes, 0.5 + gll_nodes], axis=1)
    cell_to_node = (interp_cols[None, :, None, :] * interp_cols[:, None, :, None]).reshape(16, 4)
    node_x = np.tile(gll_nodes, 4)
    node_y = np.repeat(gll_nodes, 4)
    slope_weights = 0.5 * np.stack(
        [
            np.maximum(0.0, -node_x),
            np.maximum(0.0, node_x),
            np.maximum(0.0, -node_y),
            np.maximum(0.0, node_y),
        ],
        axis=1,
    )
    return (
        cell_weights.astype(np.float32),
        cell_to_node.astype(np.float32),
        slope_weights.astype(np.float32),
    )


def node_matrix(field_count):
    _, cell_to_node, slope_weights = remap_tables()
    cells = cell_to_node.astype(np.float64) - 0.25 * slope_weights.astype(np.float64).sum(
        axis=1, keepdims=True
    )
    both = np.concatenate([cells, slope_weights], axis=1)
    full = np.einsum("nc,fg->fncg", both, np.eye(field_count)).reshape(field_count * 16, -1)
    high = full.astype(ml_dtypes.bfloat16)
    low = (full - high.astype(np.float64)).astype(ml_dtypes.bfloat16)
    return np.concatenate([high, high, low], axis=1)


def two_parts(values):
    high = values.astype(BF16)
    return high, (values - high.astype(F32)).astype(BF16)


def chunks_kernel(grp_size, cap, levels, rate_ref, forcing_ref, *out_refs):
    me = lax.axis_index("grp")
    for step in range(grp_size):
        start = pl.multiple_of((me ^ step) * cap, cap)
        out_refs[step][:levels, :] = rate_ref[:, pl.ds(start, cap)]
        out_refs[step][levels:, :] = forcing_ref[:, pl.ds(start, cap)]


def cells_kernel(gll_ref, metric_ref, mix_ref, weights_ref, out_ref):
    fields, levels, nodes, elems = gll_ref.shape
    metric = metric_ref[...]
    area = jnp.dot(
        weights_ref[...], metric, precision=lax.Precision.HIGHEST, preferred_element_type=F32
    )
    inverse = 1.0 / area
    scale = jnp.concatenate(
        [jnp.broadcast_to(inverse[c : c + 1], (fields, elems)) for c in range(4)], axis=0
    )
    high, low = two_parts(mix_ref[...])
    lhs = jnp.concatenate(
        [
            jnp.concatenate([high, high], axis=1),
            jnp.concatenate([low, jnp.zeros_like(low)], axis=1),
        ],
        axis=0,
    )
    rows = 4 * fields
    for level in range(0, levels, 2):
        pair = jnp.concatenate(
            [
                (gll_ref[:, level + k] * metric[None]).reshape(fields * nodes, elems)
                for k in range(2)
            ],
            axis=1,
        )
        pair_high, pair_low = two_parts(pair)
        res = jnp.dot(
            lhs, jnp.concatenate([pair_high, pair_low], axis=0), preferred_element_type=F32
        )
        res = res[:rows] + res[rows:]
        for k in range(2):
            out_ref[level + k] = res[:, k * elems : (k + 1) * elems] * scale


def columns_kernel(grp_size, cap, swapped, owner_ref, tri_ref, mixed_ref, *refs):
    slot_refs, (tend_ref, mean_ref, head_ref, tail_ref) = refs[:-4], refs[-4:]
    levels, rows, elems = mixed_ref.shape
    fields = rows // 4
    me = lax.axis_index("grp")
    owners = [owner_ref[c] for c in range(4)]
    pad = -(-grp_size // 8) * 8
    groups = lax.broadcasted_iota(jnp.int32, (pad, elems), 0)
    masks = [jnp.where(groups == owner, 1.0, 0.0) for owner in owners]
    before = jnp.dot(
        (masks[0] + masks[1] + masks[2] + masks[3]).astype(BF16),
        tri_ref[...],
        preferred_element_type=F32,
    )
    onehots = []
    slot_ids = lax.broadcasted_iota(jnp.int32, (grp_size * cap, elems), 0)
    for c in range(4):
        rank = jnp.sum(masks[c] * before, axis=0, keepdims=True).astype(jnp.int32)
        before = before + masks[c]
        block = (owners[c] ^ me) if swapped else owners[c]
        onehots.append(jnp.where(slot_ids == block * cap + rank, 1.0, 0.0).astype(BF16))
    onehot = jnp.concatenate(onehots, axis=1)
    slots = (
        jnp.concatenate([ref[...] for ref in slot_refs], axis=1)
        if len(slot_refs) > 1
        else slot_refs[0][...]
    )
    high, low = two_parts(slots)
    picked = jnp.dot(
        jnp.concatenate([high, low], axis=0), onehot, preferred_element_type=F32
    )
    picked = picked[: 2 * levels] + picked[2 * levels :]
    for level in range(levels):
        total = None
        for c in range(4):
            lanes = slice(c * elems, (c + 1) * elems)
            rate = picked[level : level + 1, lanes]
            forcing = picked[levels + level : levels + level + 1, lanes]
            part = rate * jnp.tanh(mixed_ref[level, c * fields : (c + 1) * fields] + forcing)
            tend_ref[level, c * fields : (c + 1) * fields] = part
            total = part if total is None else total + part
        mean_ref[level * fields : (level + 1) * fields] = 0.25 * total
    zone = lax.broadcasted_iota(jnp.int32, head_ref.shape, 1) // HALO
    parts = elems // HALO
    quarter = head_ref.shape[0]
    head = tail = None
    for j in range(parts):
        piece = mean_ref[j * quarter : (j + 1) * quarter]
        if j:
            piece = pltpu.roll(piece, j * HALO, 1)
        head = piece if head is None else jnp.where(zone == j, piece, head)
        tail = piece if tail is None else jnp.where(zone == (j + parts - 1) % parts, piece, tail)
    head_ref[...] = head
    tail_ref[...] = tail


def nodes_kernel(
    row_size, total_elems, neigh_ref, matrix_ref, tend_ref, mean_ref, left_ref, right_ref, out_ref
):
    levels, rows, elems = tend_ref.shape
    fields = rows // 4
    parts = elems // HALO
    first = (lax.axis_index("grp") * row_size + lax.axis_index("row")) * elems
    j = pl.program_id(0)
    zone = lax.broadcasted_iota(jnp.int32, left_ref.shape, 1) // HALO
    halo = jnp.where(
        zone == j,
        right_ref[...],
        jnp.where(zone == (j + parts - 1) % parts, left_ref[...], 0.0),
    )
    halo = pltpu.roll(halo, (elems - j * HALO) % elems, 1)
    high, low = two_parts(jnp.concatenate([mean_ref[...], halo], axis=1))
    places = lax.broadcasted_iota(jnp.int32, (2 * elems, elems), 0)
    onehots = []
    for k in range(4):
        local = neigh_ref[k : k + 1] - first
        local = jnp.where(local < -HALO, local + total_elems, local)
        local = jnp.where(local >= elems + HALO, local - total_elems, local)
        inside = (local >= 0) & (local < elems)
        place = jnp.where(
            inside, local, jnp.where(local < 0, local + 2 * elems, local)
        )
        onehots.append(jnp.where(places == place, 1.0, 0.0).astype(BF16))
    around = jnp.dot(
        jnp.concatenate([high, low], axis=0),
        jnp.concatenate(onehots, axis=1),
        preferred_element_type=F32,
    )
    count = high.shape[0]
    around = around[:count] + around[count:]
    matrix = matrix_ref[...]
    for level in range(0, levels, 2):
        columns = []
        for k in range(2):
            near = around[(level + k) * fields : (level + k + 1) * fields]
            columns.append(
                [tend_ref[level + k, c * fields : (c + 1) * fields] for c in range(4)]
                + [near[:, n * elems : (n + 1) * elems] for n in range(4)]
            )
        both = jnp.concatenate([jnp.concatenate(column, axis=0) for column in columns], axis=1)
        both_high, both_low = two_parts(both)
        res = jnp.dot(
            matrix,
            jnp.concatenate([both_high, both_low, both_high], axis=0),
            preferred_element_type=F32,
        )
        for k in range(2):
            lower = upper = columns[k][0]
            for value in columns[k][1:]:
                lower = jnp.minimum(lower, value)
                upper = jnp.maximum(upper, value)
            mine = res[:, k * elems : (k + 1) * elems].reshape(fields, 16, elems)
            out_ref[:, level + k] = jnp.minimum(
                jnp.maximum(mine, lower[:, None]), upper[:, None]
            )


def on_device(gll_state, metric, phys_owner, neighbours, phys_rate, phys_forcing, field_mix):
    fields, levels, nodes, elems = gll_state.shape
    grp_size = lax.axis_size("grp")
    row_size = lax.axis_size("row")
    cap = phys_rate.shape[1] // grp_size
    cell_weights, _, _ = remap_tables()
    vmem = pl.BlockSpec(memory_space=pltpu.VMEM)
    swapped = grp_size <= 16 and grp_size & (grp_size - 1) == 0 and cap % 128 == 0
    if swapped:
        chunks = pl.pallas_call(
            lambda *refs: chunks_kernel(grp_size, cap, levels, *refs),
            out_shape=[jax.ShapeDtypeStruct((2 * levels, cap), F32)] * grp_size,
            in_specs=[vmem] * 2,
            out_specs=[vmem] * grp_size,
            name="chunks",
        )(phys_rate, phys_forcing)
        slots = [chunks[0]] + [
            lax.ppermute(chunks[step], "grp", [(i, i ^ step) for i in range(grp_size)])
            for step in range(1, grp_size)
        ]
    else:
        both = jnp.concatenate([phys_rate, phys_forcing], axis=0)
        both = both.reshape(2 * levels, grp_size, cap).transpose(1, 0, 2)
        both = lax.all_to_all(both, "grp", split_axis=0, concat_axis=0, tiled=True)
        slots = [both.transpose(1, 0, 2).reshape(2 * levels, grp_size * cap)]

    mix = jnp.einsum(
        "cn,fg->cfgn", jnp.asarray(cell_weights), field_mix, precision=lax.Precision.HIGHEST
    ).reshape(4 * fields, fields * nodes)
    block = levels // 4
    weights = np.concatenate([cell_weights, cell_weights], axis=0)
    mixed = pl.pallas_call(
        cells_kernel,
        grid=(levels // block,),
        out_shape=jax.ShapeDtypeStruct((levels, 4 * fields, elems), F32),
        in_specs=[
            pl.BlockSpec((fields, block, nodes, elems), lambda i: (0, i, 0, 0)),
            pl.BlockSpec((nodes, elems), lambda i: (0, 0)),
            pl.BlockSpec((4 * fields, fields * nodes), lambda i: (0, 0)),
            pl.BlockSpec((8, nodes), lambda i: (0, 0)),
        ],
        out_specs=pl.BlockSpec((block, 4 * fields, elems), lambda i: (i, 0, 0)),
        name="cells",
    )(gll_state, metric, mix, jnp.asarray(weights))

    strict = jnp.asarray(np.triu(np.ones((elems, elems)), 1).astype(ml_dtypes.bfloat16))
    owner = phys_owner.transpose(1, 2, 0)
    quarter = levels * fields * HALO // elems
    tend, mean, head, tail = pl.pallas_call(
        lambda *refs: columns_kernel(grp_size, cap, swapped, *refs),
        out_shape=[
            jax.ShapeDtypeStruct((levels, 4 * fields, elems), F32),
            jax.ShapeDtypeStruct((levels * fields, elems), F32),
            jax.ShapeDtypeStruct((quarter, elems), F32),
            jax.ShapeDtypeStruct((quarter, elems), F32),
        ],
        in_specs=[vmem] * (3 + len(slots)),
        out_specs=[vmem] * 4,
        name="columns",
    )(owner, strict, mixed, *slots)

    count = grp_size * row_size
    left = lax.ppermute(tail, ("grp", "row"), [(i, (i + 1) % count) for i in range(count)])
    right = lax.ppermute(head, ("grp", "row"), [((i + 1) % count, i) for i in range(count)])

    matrix = jnp.asarray(node_matrix(fields))
    return pl.pallas_call(
        lambda *refs: nodes_kernel(row_size, count * elems, *refs),
        grid=(levels // block,),
        out_shape=jax.ShapeDtypeStruct(gll_state.shape, F32),
        in_specs=[
            pl.BlockSpec((4, elems), lambda i: (0, 0)),
            pl.BlockSpec(matrix.shape, lambda i: (0, 0)),
            pl.BlockSpec((block, 4 * fields, elems), lambda i: (i, 0, 0)),
            pl.BlockSpec((block * fields, elems), lambda i: (i, 0)),
            pl.BlockSpec((quarter, elems), lambda i: (0, 0)),
            pl.BlockSpec((quarter, elems), lambda i: (0, 0)),
        ],
        out_specs=pl.BlockSpec((fields, block, nodes, elems), lambda i: (0, i, 0, 0)),
        name="nodes",
    )(neighbours, matrix, tend, mean, left, right)


def solution(mesh):
    in_specs = (
        P(None, None, None, ("grp", "row")),
        P(None, ("grp", "row")),
        P(("grp", "row"), None, None),
        P(None, ("grp", "row")),
        P(None, ("grp", "row")),
        P(None, ("grp", "row")),
        P(),
    )
    out_specs = P(None, None, None, ("grp", "row"))
    return jax.shard_map(
        on_device, mesh=mesh, in_specs=in_specs, out_specs=out_specs, check_vma=False
    )
```

```python
import jax
import jax.numpy as jnp
import ml_dtypes
import numpy as np
from jax import lax
from jax.experimental import pallas as pl
from jax.experimental.pallas import tpu as pltpu
from jax.sharding import PartitionSpec as P

HALO = 32
ALIGNED = True
BF16 = jnp.bfloat16
F32 = jnp.float32
SMALL_GRANT = pltpu.CompilerParams(vmem_limit_bytes=16 << 20)


def lagrange_value(gll_nodes, node_index, point):
    value = 1.0
    for other_index in range(4):
        if other_index != node_index:
            value = (
                value
                * (point - gll_nodes[other_index])
                / (gll_nodes[node_index] - gll_nodes[other_index])
            )
    return value


def remap_tables():
    gll_nodes = np.array([-1.0, -1.0 / np.sqrt(5.0), 1.0 / np.sqrt(5.0), 1.0])
    offset = 0.5 / np.sqrt(3.0)
    halves = np.zeros((2, 4))
    for node_index in range(4):
        left_sum = lagrange_value(gll_nodes, node_index, -0.5 - offset) + lagrange_value(
            gll_nodes, node_index, -0.5 + offset
        )
        right_sum = lagrange_value(gll_nodes, node_index, 0.5 - offset) + lagrange_value(
            gll_nodes, node_index, 0.5 + offset
        )
        halves[0, node_index] = 0.5 * left_sum
        halves[1, node_index] = 0.5 * right_sum
    cell_weights = (halves[None, :, None, :] * halves[:, None, :, None]).reshape(4, 16)
    interp_cols = np.stack([0.5 - gll_nodes, 0.5 + gll_nodes], axis=1)
    cell_to_node = (interp_cols[None, :, None, :] * interp_cols[:, None, :, None]).reshape(16, 4)
    node_x = np.tile(gll_nodes, 4)
    node_y = np.repeat(gll_nodes, 4)
    slope_weights = 0.5 * np.stack(
        [
            np.maximum(0.0, -node_x),
            np.maximum(0.0, node_x),
            np.maximum(0.0, -node_y),
            np.maximum(0.0, node_y),
        ],
        axis=1,
    )
    return (
        cell_weights.astype(np.float32),
        cell_to_node.astype(np.float32),
        slope_weights.astype(np.float32),
    )


def node_matrix(field_count):
    _, cell_to_node, slope_weights = remap_tables()
    cells = cell_to_node.astype(np.float64) - 0.25 * slope_weights.astype(np.float64).sum(
        axis=1, keepdims=True
    )
    both = np.concatenate([cells, slope_weights], axis=1)
    full = np.einsum("nc,fg->fncg", both, np.eye(field_count)).reshape(field_count * 16, -1)
    high = full.astype(ml_dtypes.bfloat16)
    low = (full - high.astype(np.float64)).astype(ml_dtypes.bfloat16)
    return np.concatenate([high, high, low], axis=1)


def two_parts(values):
    high = values.astype(BF16)
    return high, (values - high.astype(F32)).astype(BF16)


def chunks_kernel(grp_size, cap, levels, rate_ref, forcing_ref, *out_refs):
    me = lax.axis_index("grp")
    for step in range(grp_size):
        start = pl.multiple_of((me ^ step) * cap, cap)
        out_refs[step][:levels, :] = rate_ref[:, pl.ds(start, cap)]
        out_refs[step][levels:, :] = forcing_ref[:, pl.ds(start, cap)]


def blocks_kernel(grp_size, cap, levels, rate_ref, forcing_ref, out_ref):
    for g in range(grp_size):
        out_ref[g, :levels] = rate_ref[:, g * cap : (g + 1) * cap]
        out_ref[g, levels:] = forcing_ref[:, g * cap : (g + 1) * cap]


def cells_kernel(gll_ref, metric_ref, mix_ref, weights_ref, out_ref):
    fields, levels, nodes, elems = gll_ref.shape
    metric = metric_ref[...]
    area = jnp.dot(
        weights_ref[...], metric, precision=lax.Precision.HIGHEST, preferred_element_type=F32
    )
    inverse = 1.0 / area
    scale = jnp.concatenate(
        [jnp.broadcast_to(inverse[c : c + 1], (fields, elems)) for c in range(4)], axis=0
    )
    high, low = two_parts(mix_ref[...])
    lhs = jnp.concatenate(
        [
            jnp.concatenate([high, high], axis=1),
            jnp.concatenate([low, jnp.zeros_like(low)], axis=1),
        ],
        axis=0,
    )
    rows = 4 * fields
    for level in range(0, levels, 2):
        pair = jnp.concatenate(
            [
                (gll_ref[:, level + k] * metric[None]).reshape(fields * nodes, elems)
                for k in range(2)
            ],
            axis=1,
        )
        pair_high, pair_low = two_parts(pair)
        res = jnp.dot(
            lhs, jnp.concatenate([pair_high, pair_low], axis=0), preferred_element_type=F32
        )
        res = res[:rows] + res[rows:]
        for k in range(2):
            out_ref[level + k] = res[:, k * elems : (k + 1) * elems] * scale


def columns_kernel(grp_size, cap, swapped, owner_ref, tri_ref, mixed_ref, *refs):
    slot_refs, (tend_ref, mean_ref, head_ref, tail_ref) = refs[:-4], refs[-4:]
    levels, rows, elems = mixed_ref.shape
    fields = rows // 4
    me = lax.axis_index("grp")
    owners = [owner_ref[c] for c in range(4)]
    pad = -(-grp_size // 8) * 8
    groups = lax.broadcasted_iota(jnp.int32, (pad, elems), 0)
    masks = [jnp.where(groups == owner, 1.0, 0.0) for owner in owners]
    before = jnp.dot(
        (masks[0] + masks[1] + masks[2] + masks[3]).astype(BF16),
        tri_ref[...],
        preferred_element_type=F32,
    )
    onehots = []
    slot_ids = lax.broadcasted_iota(jnp.int32, (grp_size * cap, elems), 0)
    for c in range(4):
        rank = jnp.sum(masks[c] * before, axis=0, keepdims=True).astype(jnp.int32)
        before = before + masks[c]
        block = (owners[c] ^ me) if swapped else owners[c]
        onehots.append(jnp.where(slot_ids == block * cap + rank, 1.0, 0.0).astype(BF16))
    onehot = jnp.concatenate(onehots, axis=1)
    if len(slot_refs) > 1:
        slots = jnp.concatenate([ref[...] for ref in slot_refs], axis=1)
    elif len(slot_refs[0].shape) > 2:
        slots = jnp.concatenate([slot_refs[0][g] for g in range(grp_size)], axis=1)
    else:
        slots = slot_refs[0][...]
    high, low = two_parts(slots)
    picked = jnp.dot(
        jnp.concatenate([high, low], axis=0), onehot, preferred_element_type=F32
    )
    picked = picked[: 2 * levels] + picked[2 * levels :]
    for level in range(levels):
        total = None
        for c in range(4):
            lanes = slice(c * elems, (c + 1) * elems)
            rate = picked[level : level + 1, lanes]
            forcing = picked[levels + level : levels + level + 1, lanes]
            part = rate * jnp.tanh(mixed_ref[level, c * fields : (c + 1) * fields] + forcing)
            tend_ref[level, c * fields : (c + 1) * fields] = part
            total = part if total is None else total + part
        mean_ref[level * fields : (level + 1) * fields] = 0.25 * total
    zone = lax.broadcasted_iota(jnp.int32, head_ref.shape, 1) // HALO
    parts = elems // HALO
    quarter = head_ref.shape[0]
    head = tail = None
    for j in range(parts):
        piece = mean_ref[j * quarter : (j + 1) * quarter]
        if j:
            piece = pltpu.roll(piece, j * HALO, 1)
        head = piece if head is None else jnp.where(zone == j, piece, head)
        tail = piece if tail is None else jnp.where(zone == (j + parts - 1) % parts, piece, tail)
    head_ref[...] = head
    tail_ref[...] = tail


def nodes_kernel(
    row_size, total_elems, neigh_ref, matrix_ref, tend_ref, mean_ref, left_ref, right_ref, out_ref
):
    levels, rows, elems = tend_ref.shape
    fields = rows // 4
    parts = elems // HALO
    first = (lax.axis_index("grp") * row_size + lax.axis_index("row")) * elems
    j = pl.program_id(0)
    zone = lax.broadcasted_iota(jnp.int32, left_ref.shape, 1) // HALO
    halo = jnp.where(
        zone == j,
        right_ref[...],
        jnp.where(zone == (j + parts - 1) % parts, left_ref[...], 0.0),
    )
    halo = pltpu.roll(halo, (elems - j * HALO) % elems, 1)
    high, low = two_parts(jnp.concatenate([mean_ref[...], halo], axis=1))
    places = lax.broadcasted_iota(jnp.int32, (2 * elems, elems), 0)
    onehots = []
    for k in range(4):
        local = neigh_ref[k : k + 1] - first
        local = jnp.where(local < -HALO, local + total_elems, local)
        local = jnp.where(local >= elems + HALO, local - total_elems, local)
        inside = (local >= 0) & (local < elems)
        place = jnp.where(
            inside, local, jnp.where(local < 0, local + 2 * elems, local)
        )
        onehots.append(jnp.where(places == place, 1.0, 0.0).astype(BF16))
    around = jnp.dot(
        jnp.concatenate([high, low], axis=0),
        jnp.concatenate(onehots, axis=1),
        preferred_element_type=F32,
    )
    count = high.shape[0]
    around = around[:count] + around[count:]
    matrix = matrix_ref[...]
    for level in range(0, levels, 2):
        columns = []
        for k in range(2):
            near = around[(level + k) * fields : (level + k + 1) * fields]
            columns.append(
                [tend_ref[level + k, c * fields : (c + 1) * fields] for c in range(4)]
                + [near[:, n * elems : (n + 1) * elems] for n in range(4)]
            )
        both = jnp.concatenate([jnp.concatenate(column, axis=0) for column in columns], axis=1)
        both_high, both_low = two_parts(both)
        res = jnp.dot(
            matrix,
            jnp.concatenate([both_high, both_low, both_high], axis=0),
            preferred_element_type=F32,
        )
        for k in range(2):
            lower = upper = columns[k][0]
            for value in columns[k][1:]:
                lower = jnp.minimum(lower, value)
                upper = jnp.maximum(upper, value)
            mine = res[:, k * elems : (k + 1) * elems].reshape(fields, 16, elems)
            out_ref[:, level + k] = jnp.minimum(
                jnp.maximum(mine, lower[:, None]), upper[:, None]
            )


def on_device(gll_state, metric, phys_owner, neighbours, phys_rate, phys_forcing, field_mix):
    fields, levels, nodes, elems = gll_state.shape
    grp_size = lax.axis_size("grp")
    row_size = lax.axis_size("row")
    cap = phys_rate.shape[1] // grp_size
    cell_weights, _, _ = remap_tables()
    vmem = pl.BlockSpec(memory_space=pltpu.VMEM)
    swapped = not ALIGNED and grp_size <= 16 and grp_size & (grp_size - 1) == 0 and cap % 128 == 0
    if swapped:
        chunks = pl.pallas_call(
            lambda *refs: chunks_kernel(grp_size, cap, levels, *refs),
            out_shape=[jax.ShapeDtypeStruct((2 * levels, cap), F32)] * grp_size,
            in_specs=[vmem] * 2,
            out_specs=[vmem] * grp_size,
            compiler_params=SMALL_GRANT,
        name="chunks",
        )(phys_rate, phys_forcing)
        slots = [chunks[0]] + [
            lax.ppermute(chunks[step], "grp", [(i, i ^ step) for i in range(grp_size)])
            for step in range(1, grp_size)
        ]
    else:
        both = jnp.concatenate([phys_rate, phys_forcing], axis=0)
        both = both.reshape(2 * levels, grp_size, cap).transpose(1, 0, 2)
        both = lax.all_to_all(both, "grp", split_axis=0, concat_axis=0, tiled=True)
        slots = [both.transpose(1, 0, 2).reshape(2 * levels, grp_size * cap)]
    if ALIGNED and cap % 128 == 0:
        both = pl.pallas_call(
            lambda *refs: blocks_kernel(grp_size, cap, levels, *refs),
            out_shape=jax.ShapeDtypeStruct((grp_size, 2 * levels, cap), F32),
            in_specs=[vmem] * 2,
            out_specs=vmem,
            compiler_params=SMALL_GRANT,
            name="blocks",
        )(phys_rate, phys_forcing)
        both = lax.all_to_all(both, "grp", split_axis=0, concat_axis=0, tiled=True)
        slots = [both]

    mix = jnp.einsum(
        "cn,fg->cfgn", jnp.asarray(cell_weights), field_mix, precision=lax.Precision.HIGHEST
    ).reshape(4 * fields, fields * nodes)
    block = levels // 4
    weights = np.concatenate([cell_weights, cell_weights], axis=0)
    mixed = pl.pallas_call(
        cells_kernel,
        grid=(levels // block,),
        out_shape=jax.ShapeDtypeStruct((levels, 4 * fields, elems), F32),
        in_specs=[
            pl.BlockSpec((fields, block, nodes, elems), lambda i: (0, i, 0, 0)),
            pl.BlockSpec((nodes, elems), lambda i: (0, 0)),
            pl.BlockSpec((4 * fields, fields * nodes), lambda i: (0, 0)),
            pl.BlockSpec((8, nodes), lambda i: (0, 0)),
        ],
        out_specs=pl.BlockSpec((block, 4 * fields, elems), lambda i: (i, 0, 0)),
        compiler_params=SMALL_GRANT,
        name="cells",
    )(gll_state, metric, mix, jnp.asarray(weights))

    strict = jnp.asarray(np.triu(np.ones((elems, elems)), 1).astype(ml_dtypes.bfloat16))
    owner = phys_owner.transpose(1, 2, 0)
    quarter = levels * fields * HALO // elems
    tend, mean, head, tail = pl.pallas_call(
        lambda *refs: columns_kernel(grp_size, cap, swapped, *refs),
        out_shape=[
            jax.ShapeDtypeStruct((levels, 4 * fields, elems), F32),
            jax.ShapeDtypeStruct((levels * fields, elems), F32),
            jax.ShapeDtypeStruct((quarter, elems), F32),
            jax.ShapeDtypeStruct((quarter, elems), F32),
        ],
        in_specs=[vmem] * (3 + len(slots)),
        out_specs=[vmem] * 4,
        compiler_params=SMALL_GRANT,
        name="columns",
    )(owner, strict, mixed, *slots)

    count = grp_size * row_size
    left = lax.ppermute(tail, ("grp", "row"), [(i, (i + 1) % count) for i in range(count)])
    right = lax.ppermute(head, ("grp", "row"), [((i + 1) % count, i) for i in range(count)])

    matrix = jnp.asarray(node_matrix(fields))
    return pl.pallas_call(
        lambda *refs: nodes_kernel(row_size, count * elems, *refs),
        grid=(levels // block,),
        out_shape=jax.ShapeDtypeStruct(gll_state.shape, F32),
        in_specs=[
            pl.BlockSpec((4, elems), lambda i: (0, 0)),
            pl.BlockSpec(matrix.shape, lambda i: (0, 0)),
            pl.BlockSpec((block, 4 * fields, elems), lambda i: (i, 0, 0)),
            pl.BlockSpec((block * fields, elems), lambda i: (i, 0)),
            pl.BlockSpec((quarter, elems), lambda i: (0, 0)),
            pl.BlockSpec((quarter, elems), lambda i: (0, 0)),
        ],
        out_specs=pl.BlockSpec((fields, block, nodes, elems), lambda i: (0, i, 0, 0)),
        compiler_params=SMALL_GRANT,
        name="nodes",
    )(neighbours, matrix, tend, mean, left, right)


def solution(mesh):
    in_specs = (
        P(None, None, None, ("grp", "row")),
        P(None, ("grp", "row")),
        P(("grp", "row"), None, None),
        P(None, ("grp", "row")),
        P(None, ("grp", "row")),
        P(None, ("grp", "row")),
        P(),
    )
    out_specs = P(None, None, None, ("grp", "row"))
    return jax.shard_map(
        on_device, mesh=mesh, in_specs=in_specs, out_specs=out_specs, check_vma=False
    )
```

```python
import jax
import jax.numpy as jnp
import ml_dtypes
import numpy as np
from jax import lax
from jax.experimental import pallas as pl
from jax.experimental.pallas import tpu as pltpu
from jax.sharding import PartitionSpec as P

HALO = 32
ALIGNED = True
BF16 = jnp.bfloat16
F32 = jnp.float32
SMALL_GRANT = pltpu.CompilerParams(vmem_limit_bytes=16 << 20)


def lagrange_value(gll_nodes, node_index, point):
    value = 1.0
    for other_index in range(4):
        if other_index != node_index:
            value = (
                value
                * (point - gll_nodes[other_index])
                / (gll_nodes[node_index] - gll_nodes[other_index])
            )
    return value


def remap_tables():
    gll_nodes = np.array([-1.0, -1.0 / np.sqrt(5.0), 1.0 / np.sqrt(5.0), 1.0])
    offset = 0.5 / np.sqrt(3.0)
    halves = np.zeros((2, 4))
    for node_index in range(4):
        left_sum = lagrange_value(gll_nodes, node_index, -0.5 - offset) + lagrange_value(
            gll_nodes, node_index, -0.5 + offset
        )
        right_sum = lagrange_value(gll_nodes, node_index, 0.5 - offset) + lagrange_value(
            gll_nodes, node_index, 0.5 + offset
        )
        halves[0, node_index] = 0.5 * left_sum
        halves[1, node_index] = 0.5 * right_sum
    cell_weights = (halves[None, :, None, :] * halves[:, None, :, None]).reshape(4, 16)
    interp_cols = np.stack([0.5 - gll_nodes, 0.5 + gll_nodes], axis=1)
    cell_to_node = (interp_cols[None, :, None, :] * interp_cols[:, None, :, None]).reshape(16, 4)
    node_x = np.tile(gll_nodes, 4)
    node_y = np.repeat(gll_nodes, 4)
    slope_weights = 0.5 * np.stack(
        [
            np.maximum(0.0, -node_x),
            np.maximum(0.0, node_x),
            np.maximum(0.0, -node_y),
            np.maximum(0.0, node_y),
        ],
        axis=1,
    )
    return (
        cell_weights.astype(np.float32),
        cell_to_node.astype(np.float32),
        slope_weights.astype(np.float32),
    )


def node_matrix(field_count):
    _, cell_to_node, slope_weights = remap_tables()
    cells = cell_to_node.astype(np.float64) - 0.25 * slope_weights.astype(np.float64).sum(
        axis=1, keepdims=True
    )
    both = np.concatenate([cells, slope_weights], axis=1)
    full = np.einsum("nc,fg->fncg", both, np.eye(field_count)).reshape(field_count * 16, -1)
    high = full.astype(ml_dtypes.bfloat16)
    low = (full - high.astype(np.float64)).astype(ml_dtypes.bfloat16)
    return np.concatenate([high, high, low], axis=1)


def two_parts(values):
    high = values.astype(BF16)
    return high, (values - high.astype(F32)).astype(BF16)


def chunks_kernel(grp_size, cap, levels, rate_ref, forcing_ref, *out_refs):
    me = lax.axis_index("grp")
    for step in range(grp_size):
        start = pl.multiple_of((me ^ step) * cap, cap)
        out_refs[step][:levels, :] = rate_ref[:, pl.ds(start, cap)]
        out_refs[step][levels:, :] = forcing_ref[:, pl.ds(start, cap)]


def blocks_kernel(grp_size, cap, levels, rate_ref, forcing_ref, out_ref, sems):
    copies = []
    for g in range(grp_size):
        for k, ref in enumerate((rate_ref, forcing_ref)):
            copies.append(
                pltpu.make_async_copy(
                    ref.at[:, pl.ds(g * cap, cap)],
                    out_ref.at[g, pl.ds(k * levels, levels)],
                    sems.at[2 * g + k],
                )
            )
    for copy in copies:
        copy.start()
    for copy in copies:
        copy.wait()


def cells_kernel(gll_ref, metric_ref, mix_ref, weights_ref, out_ref):
    fields, levels, nodes, elems = gll_ref.shape
    metric = metric_ref[...]
    area = jnp.dot(
        weights_ref[...], metric, precision=lax.Precision.HIGHEST, preferred_element_type=F32
    )
    inverse = 1.0 / area
    scale = jnp.concatenate(
        [jnp.broadcast_to(inverse[c : c + 1], (fields, elems)) for c in range(4)], axis=0
    )
    high, low = two_parts(mix_ref[...])
    lhs = jnp.concatenate(
        [
            jnp.concatenate([high, high], axis=1),
            jnp.concatenate([low, jnp.zeros_like(low)], axis=1),
        ],
        axis=0,
    )
    rows = 4 * fields
    for level in range(0, levels, 2):
        pair = jnp.concatenate(
            [
                (gll_ref[:, level + k] * metric[None]).reshape(fields * nodes, elems)
                for k in range(2)
            ],
            axis=1,
        )
        pair_high, pair_low = two_parts(pair)
        res = jnp.dot(
            lhs, jnp.concatenate([pair_high, pair_low], axis=0), preferred_element_type=F32
        )
        res = res[:rows] + res[rows:]
        for k in range(2):
            out_ref[level + k] = res[:, k * elems : (k + 1) * elems] * scale


def columns_kernel(grp_size, cap, swapped, owner_ref, tri_ref, mixed_ref, *refs):
    slot_refs, (tend_ref, mean_ref, head_ref, tail_ref) = refs[:-4], refs[-4:]
    levels, rows, elems = mixed_ref.shape
    fields = rows // 4
    me = lax.axis_index("grp")
    owners = [owner_ref[c] for c in range(4)]
    pad = -(-grp_size // 8) * 8
    groups = lax.broadcasted_iota(jnp.int32, (pad, elems), 0)
    masks = [jnp.where(groups == owner, 1.0, 0.0) for owner in owners]
    before = jnp.dot(
        (masks[0] + masks[1] + masks[2] + masks[3]).astype(BF16),
        tri_ref[...],
        preferred_element_type=F32,
    )
    onehots = []
    slot_ids = lax.broadcasted_iota(jnp.int32, (grp_size * cap, elems), 0)
    for c in range(4):
        rank = jnp.sum(masks[c] * before, axis=0, keepdims=True).astype(jnp.int32)
        before = before + masks[c]
        block = (owners[c] ^ me) if swapped else owners[c]
        onehots.append(jnp.where(slot_ids == block * cap + rank, 1.0, 0.0).astype(BF16))
    onehot = jnp.concatenate(onehots, axis=1)
    if len(slot_refs) > 1:
        slots = jnp.concatenate([ref[...] for ref in slot_refs], axis=1)
    elif len(slot_refs[0].shape) > 2:
        slots = jnp.concatenate([slot_refs[0][g] for g in range(grp_size)], axis=1)
    else:
        slots = slot_refs[0][...]
    high, low = two_parts(slots)
    picked = jnp.dot(
        jnp.concatenate([high, low], axis=0), onehot, preferred_element_type=F32
    )
    picked = picked[: 2 * levels] + picked[2 * levels :]
    for level in range(levels):
        total = None
        for c in range(4):
            lanes = slice(c * elems, (c + 1) * elems)
            rate = picked[level : level + 1, lanes]
            forcing = picked[levels + level : levels + level + 1, lanes]
            part = rate * jnp.tanh(mixed_ref[level, c * fields : (c + 1) * fields] + forcing)
            tend_ref[level, c * fields : (c + 1) * fields] = part
            total = part if total is None else total + part
        mean_ref[level * fields : (level + 1) * fields] = 0.25 * total
    zone = lax.broadcasted_iota(jnp.int32, head_ref.shape, 1) // HALO
    parts = elems // HALO
    quarter = head_ref.shape[0]
    head = tail = None
    for j in range(parts):
        piece = mean_ref[j * quarter : (j + 1) * quarter]
        if j:
            piece = pltpu.roll(piece, j * HALO, 1)
        head = piece if head is None else jnp.where(zone == j, piece, head)
        tail = piece if tail is None else jnp.where(zone == (j + parts - 1) % parts, piece, tail)
    head_ref[...] = head
    tail_ref[...] = tail


def inner_kernel(
    row_size, total_elems, neigh_ref, tend_ref, mean_ref, near_ref, place_ref, lower_ref, upper_ref
):
    levels, rows, elems = tend_ref.shape
    fields = rows // 4
    first = (lax.axis_index("grp") * row_size + lax.axis_index("row")) * elems
    places = lax.broadcasted_iota(jnp.int32, (elems, elems), 0)
    own, outer = [], []
    for k in range(4):
        local = neigh_ref[k : k + 1] - first
        local = jnp.where(local < -HALO, local + total_elems, local)
        local = jnp.where(local >= elems + HALO, local - total_elems, local)
        inside = (local >= 0) & (local < elems)
        wrapped = jnp.where(
            local < 0, local + elems, jnp.where(local >= elems, local - elems, local)
        )
        own.append(jnp.where(places == jnp.where(inside, local, -1), 1.0, 0.0).astype(BF16))
        outer.append(jnp.where(places == jnp.where(inside, -1, wrapped), 1.0, 0.0).astype(BF16))
    place_ref[...] = jnp.concatenate(outer, axis=1)
    high, low = two_parts(mean_ref[...])
    own = jnp.concatenate(own, axis=1)
    near_ref[...] = jnp.dot(high, own, preferred_element_type=F32) + jnp.dot(
        low, own, preferred_element_type=F32
    )
    for level in range(levels):
        lower = upper = tend_ref[level, :fields]
        for c in range(1, 4):
            value = tend_ref[level, c * fields : (c + 1) * fields]
            lower = jnp.minimum(lower, value)
            upper = jnp.maximum(upper, value)
        lower_ref[level * fields : (level + 1) * fields] = lower
        upper_ref[level * fields : (level + 1) * fields] = upper


def nodes_kernel(
    matrix_ref,
    tend_ref,
    near_ref,
    place_ref,
    lower_ref,
    upper_ref,
    left_ref,
    right_ref,
    out_ref,
):
    levels, rows, elems = tend_ref.shape
    fields = rows // 4
    parts = elems // HALO
    j = pl.program_id(0)
    zone = lax.broadcasted_iota(jnp.int32, left_ref.shape, 1) // HALO
    halo = jnp.where(
        zone == j,
        right_ref[...],
        jnp.where(zone == (j + parts - 1) % parts, left_ref[...], 0.0),
    )
    halo = pltpu.roll(halo, (elems - j * HALO) % elems, 1)
    high, low = two_parts(halo)
    around = jnp.dot(
        jnp.concatenate([high, low], axis=0), place_ref[...], preferred_element_type=F32
    )
    count = high.shape[0]
    around = around[:count] + around[count:] + near_ref[...]
    matrix = matrix_ref[...]
    for level in range(0, levels, 2):
        columns = []
        for k in range(2):
            near = around[(level + k) * fields : (level + k + 1) * fields]
            columns.append(
                [tend_ref[level + k, c * fields : (c + 1) * fields] for c in range(4)]
                + [near[:, n * elems : (n + 1) * elems] for n in range(4)]
            )
        both = jnp.concatenate([jnp.concatenate(column, axis=0) for column in columns], axis=1)
        both_high, both_low = two_parts(both)
        res = jnp.dot(
            matrix,
            jnp.concatenate([both_high, both_low, both_high], axis=0),
            preferred_element_type=F32,
        )
        for k in range(2):
            lower = lower_ref[(level + k) * fields : (level + k + 1) * fields]
            upper = upper_ref[(level + k) * fields : (level + k + 1) * fields]
            for value in columns[k][4:]:
                lower = jnp.minimum(lower, value)
                upper = jnp.maximum(upper, value)
            mine = res[:, k * elems : (k + 1) * elems].reshape(fields, 16, elems)
            out_ref[:, level + k] = jnp.minimum(
                jnp.maximum(mine, lower[:, None]), upper[:, None]
            )


def on_device(gll_state, metric, phys_owner, neighbours, phys_rate, phys_forcing, field_mix):
    fields, levels, nodes, elems = gll_state.shape
    grp_size = lax.axis_size("grp")
    row_size = lax.axis_size("row")
    cap = phys_rate.shape[1] // grp_size
    cell_weights, _, _ = remap_tables()
    vmem = pl.BlockSpec(memory_space=pltpu.VMEM)
    swapped = not ALIGNED and grp_size <= 16 and grp_size & (grp_size - 1) == 0 and cap % 128 == 0
    if swapped:
        chunks = pl.pallas_call(
            lambda *refs: chunks_kernel(grp_size, cap, levels, *refs),
            out_shape=[jax.ShapeDtypeStruct((2 * levels, cap), F32)] * grp_size,
            in_specs=[vmem] * 2,
            out_specs=[vmem] * grp_size,
            compiler_params=SMALL_GRANT,
        name="chunks",
        )(phys_rate, phys_forcing)
        slots = [chunks[0]] + [
            lax.ppermute(chunks[step], "grp", [(i, i ^ step) for i in range(grp_size)])
            for step in range(1, grp_size)
        ]
    else:
        both = jnp.concatenate([phys_rate, phys_forcing], axis=0)
        both = both.reshape(2 * levels, grp_size, cap).transpose(1, 0, 2)
        both = lax.all_to_all(both, "grp", split_axis=0, concat_axis=0, tiled=True)
        slots = [both.transpose(1, 0, 2).reshape(2 * levels, grp_size * cap)]
    if ALIGNED and cap % 128 == 0:
        both = pl.pallas_call(
            lambda *refs: blocks_kernel(grp_size, cap, levels, *refs),
            out_shape=jax.ShapeDtypeStruct((grp_size, 2 * levels, cap), F32),
            in_specs=[pl.BlockSpec(memory_space=pltpu.MemorySpace.HBM)] * 2,
            out_specs=vmem,
            scratch_shapes=[pltpu.SemaphoreType.DMA((2 * grp_size,))],
            name="blocks",
        )(phys_rate, phys_forcing)
        both = lax.all_to_all(both, "grp", split_axis=0, concat_axis=0, tiled=True)
        slots = [both]

    mix = jnp.einsum(
        "cn,fg->cfgn", jnp.asarray(cell_weights), field_mix, precision=lax.Precision.HIGHEST
    ).reshape(4 * fields, fields * nodes)
    block = levels // 4
    weights = np.concatenate([cell_weights, cell_weights], axis=0)
    mixed = pl.pallas_call(
        cells_kernel,
        grid=(levels // block,),
        out_shape=jax.ShapeDtypeStruct((levels, 4 * fields, elems), F32),
        in_specs=[
            pl.BlockSpec((fields, block, nodes, elems), lambda i: (0, i, 0, 0)),
            pl.BlockSpec((nodes, elems), lambda i: (0, 0)),
            pl.BlockSpec((4 * fields, fields * nodes), lambda i: (0, 0)),
            pl.BlockSpec((8, nodes), lambda i: (0, 0)),
        ],
        out_specs=pl.BlockSpec((block, 4 * fields, elems), lambda i: (i, 0, 0)),
        compiler_params=SMALL_GRANT,
        name="cells",
    )(gll_state, metric, mix, jnp.asarray(weights))

    strict = jnp.asarray(np.triu(np.ones((elems, elems)), 1).astype(ml_dtypes.bfloat16))
    owner = phys_owner.transpose(1, 2, 0)
    quarter = levels * fields * HALO // elems
    tend, mean, head, tail = pl.pallas_call(
        lambda *refs: columns_kernel(grp_size, cap, swapped, *refs),
        out_shape=[
            jax.ShapeDtypeStruct((levels, 4 * fields, elems), F32),
            jax.ShapeDtypeStruct((levels * fields, elems), F32),
            jax.ShapeDtypeStruct((quarter, elems), F32),
            jax.ShapeDtypeStruct((quarter, elems), F32),
        ],
        in_specs=[vmem] * (3 + len(slots)),
        out_specs=[vmem] * 4,
        compiler_params=SMALL_GRANT,
        name="columns",
    )(owner, strict, mixed, *slots)

    count = grp_size * row_size
    left = lax.ppermute(tail, ("grp", "row"), [(i, (i + 1) % count) for i in range(count)])
    right = lax.ppermute(head, ("grp", "row"), [((i + 1) % count, i) for i in range(count)])

    near, place, lower, upper = pl.pallas_call(
        lambda *refs: inner_kernel(row_size, count * elems, *refs),
        out_shape=[
            jax.ShapeDtypeStruct((levels * fields, 4 * elems), F32),
            jax.ShapeDtypeStruct((elems, 4 * elems), BF16),
            jax.ShapeDtypeStruct((levels * fields, elems), F32),
            jax.ShapeDtypeStruct((levels * fields, elems), F32),
        ],
        in_specs=[vmem] * 3,
        out_specs=[vmem] * 4,
        compiler_params=SMALL_GRANT,
        name="inner",
    )(neighbours, tend, mean)

    matrix = jnp.asarray(node_matrix(fields))
    return pl.pallas_call(
        nodes_kernel,
        grid=(levels // block,),
        out_shape=jax.ShapeDtypeStruct(gll_state.shape, F32),
        in_specs=[
            pl.BlockSpec(matrix.shape, lambda i: (0, 0)),
            pl.BlockSpec((block, 4 * fields, elems), lambda i: (i, 0, 0)),
            pl.BlockSpec((block * fields, 4 * elems), lambda i: (i, 0)),
            pl.BlockSpec((elems, 4 * elems), lambda i: (0, 0)),
            pl.BlockSpec((block * fields, elems), lambda i: (i, 0)),
            pl.BlockSpec((block * fields, elems), lambda i: (i, 0)),
            pl.BlockSpec((quarter, elems), lambda i: (0, 0)),
            pl.BlockSpec((quarter, elems), lambda i: (0, 0)),
        ],
        out_specs=pl.BlockSpec((fields, block, nodes, elems), lambda i: (0, i, 0, 0)),
        compiler_params=SMALL_GRANT,
        name="nodes",
    )(matrix, tend, near, place, lower, upper, left, right)


def solution(mesh):
    in_specs = (
        P(None, None, None, ("grp", "row")),
        P(None, ("grp", "row")),
        P(("grp", "row"), None, None),
        P(None, ("grp", "row")),
        P(None, ("grp", "row")),
        P(None, ("grp", "row")),
        P(),
    )
    out_specs = P(None, None, None, ("grp", "row"))
    return jax.shard_map(
        on_device, mesh=mesh, in_specs=in_specs, out_specs=out_specs, check_vma=False
    )
```
